32 devices in a mesh: dp: 2 (over x), cp: 4 (over z), tp: 4 (over y, core).
Axes of the slice: x: 2, y: 2, z: 4, core: 2. Of those that a mesh axis runs over, the one named last changes fastest.
Arguments:
- x: bfloat16 [2, 8192, 3072], P('dp', ('cp', 'tp')), parts along dimension 0
- g_attn: bfloat16 [3072], replicated
- w_q: bfloat16 [3072, 24, 128], P(None, 'tp')
- w_k: bfloat16 [3072, 8, 128], P(None, 'tp')
- w_v: bfloat16 [3072, 8, 128], P(None, 'tp')
- w_o: bfloat16 [24, 128, 3072], P('tp')
- g_mlp: bfloat16 [3072], replicated
- w_gate: bfloat16 [3072, 8192], P(None, 'tp')
- w_up: bfloat16 [3072, 8192], P(None, 'tp')
- w_down: bfloat16 [8192, 3072], P('tp')
Outputs:
- output: bfloat16 [2, 8192, 3072], P('dp', ('cp', 'tp')), parts along dimension 0
There are 2 independent parts. The reference program is written for one: setup_inputs(seed, part) draws one part's arguments, and reference() takes and returns one part's arrays. A program takes and returns all parts, laid end to end along the dimension named above; an argument that names none is the same for every part.
All inputs are finite; a program needn't handle non-finite values.
Results may differ from the reference program's by a relative error of at most 0.02.
Values are sent between devices in bfloat16 or wider.
A program may use at most 1 GiB of HBM per device.

```python
import math
import jax
import jax.numpy as jnp
from jax import lax

SEQ_LEN = 8192
MODEL_DIM = 3072
N_HEADS = 24
N_KV_HEADS = 8
HEAD_DIM = 128
FFN_DIM = 8192
CP_SIZE = 4
Q_BLOCK = 128
NORM_EPS = 1e-5
ROPE_THETA = 500000.0


def stored_positions(row_ids):
    piece_len = SEQ_LEN // (2 * CP_SIZE)
    owner_cp = row_ids // (2 * piece_len)
    within = row_ids % (2 * piece_len)
    return jnp.where(within < piece_len, owner_cp * piece_len + within,
                     (2 * CP_SIZE - 1 - owner_cp) * piece_len + within - piece_len)


def rms_norm(rows_in, gain_vec):
    rows_f32 = rows_in.astype(jnp.float32)
    mean_sq = jnp.mean(rows_f32 * rows_f32, axis=-1, keepdims=True)
    return (rows_f32 * lax.rsqrt(mean_sq + NORM_EPS) * gain_vec.astype(jnp.float32)).astype(jnp.bfloat16)


def apply_rope(heads_in, positions):
    half_dim = HEAD_DIM // 2
    inv_freq = ROPE_THETA ** (-2.0 * jnp.arange(half_dim, dtype=jnp.float32) / HEAD_DIM)
    angles = positions.astype(jnp.float32)[:, None] * inv_freq[None, :]
    angles = jnp.concatenate([angles, angles], axis=-1)[:, None, :]
    heads_f32 = heads_in.astype(jnp.float32)
    rotated = jnp.concatenate([-heads_f32[..., half_dim:], heads_f32[..., :half_dim]], axis=-1)
    return (heads_f32 * jnp.cos(angles) + rotated * jnp.sin(angles)).astype(jnp.bfloat16)


def draw_weight(key_in, weight_shape, std_dev):
    return (std_dev * jax.random.normal(key_in, weight_shape, jnp.float32)).astype(jnp.bfloat16)


def setup_inputs(seed: int = 0, part: int = 0) -> dict:
    key_list = jax.random.split(jax.random.key(seed), 10)
    qk_std = math.log(SEQ_LEN / 32.0) ** 0.25 / math.sqrt(MODEL_DIM)
    x = 0.5 * jax.random.normal(jax.random.fold_in(key_list[0], part), (1, SEQ_LEN, MODEL_DIM), jnp.float32)
    return {
        'x': x.astype(jnp.bfloat16),
        'g_attn': (0.5 + jax.random.uniform(key_list[1], (MODEL_DIM,), jnp.float32)).astype(jnp.bfloat16),
        'w_q': draw_weight(key_list[2], (MODEL_DIM, N_HEADS, HEAD_DIM), qk_std),
        'w_k': draw_weight(key_list[3], (MODEL_DIM, N_KV_HEADS, HEAD_DIM), qk_std),
        'w_v': draw_weight(key_list[4], (MODEL_DIM, N_KV_HEADS, HEAD_DIM), MODEL_DIM ** -0.5),
        'w_o': draw_weight(key_list[5], (N_HEADS, HEAD_DIM, MODEL_DIM), 2.0 * (N_HEADS * HEAD_DIM) ** -0.5),
        'g_mlp': (0.5 + jax.random.uniform(key_list[6], (MODEL_DIM,), jnp.float32)).astype(jnp.bfloat16),
        'w_gate': draw_weight(key_list[7], (MODEL_DIM, FFN_DIM), MODEL_DIM ** -0.5),
        'w_up': draw_weight(key_list[8], (MODEL_DIM, FFN_DIM), MODEL_DIM ** -0.5),
        'w_down': draw_weight(key_list[9], (FFN_DIM, MODEL_DIM), FFN_DIM ** -0.5),
    }


def reference(x, g_attn, w_q, w_k, w_v, w_o, g_mlp, w_gate, w_up, w_down):
    group_size = N_HEADS // N_KV_HEADS
    n_blocks = SEQ_LEN // Q_BLOCK
    positions = stored_positions(jnp.arange(SEQ_LEN, dtype=jnp.int32))
    x_rows = x[0]
    normed = rms_norm(x_rows, g_attn)
    q_all = jnp.dot(normed, w_q.reshape(MODEL_DIM, N_HEADS * HEAD_DIM), preferred_element_type=jnp.float32).astype(jnp.bfloat16)
    k_all = jnp.dot(normed, w_k.reshape(MODEL_DIM, N_KV_HEADS * HEAD_DIM), preferred_element_type=jnp.float32).astype(jnp.bfloat16)
    v_all = jnp.dot(normed, w_v.reshape(MODEL_DIM, N_KV_HEADS * HEAD_DIM), preferred_element_type=jnp.float32).astype(jnp.bfloat16)
    q_all = apply_rope(q_all.reshape(SEQ_LEN, N_HEADS, HEAD_DIM), positions)
    k_all = apply_rope(k_all.reshape(SEQ_LEN, N_KV_HEADS, HEAD_DIM), positions).astype(jnp.float32)
    v_all = v_all.reshape(SEQ_LEN, N_KV_HEADS, HEAD_DIM).astype(jnp.float32)
    w_o_flat = w_o.reshape(N_HEADS * HEAD_DIM, MODEL_DIM)
    score_scale = HEAD_DIM ** -0.5

    def one_block(block_in):
        q_blk, pos_blk, x_blk = block_in
        q_grp = q_blk.reshape(Q_BLOCK, N_KV_HEADS, group_size, HEAD_DIM).astype(jnp.float32)
        scores = jnp.einsum('qgrd,kgd->gqrk', q_grp, k_all) * score_scale
        visible = pos_blk[None, :, None, None] >= positions[None, None, None, :]
        scores = jnp.where(visible, scores, -1e30)
        weights = jnp.exp(scores - jnp.max(scores, axis=-1, keepdims=True))
        row_sum = jnp.sum(weights, axis=-1, keepdims=True)
        mixed_vals = jnp.einsum('gqrk,kgd->gqrd', weights.astype(jnp.bfloat16).astype(jnp.float32), v_all) / row_sum
        attn_rows = jnp.transpose(mixed_vals, (1, 0, 2, 3)).astype(jnp.bfloat16).reshape(Q_BLOCK, N_HEADS * HEAD_DIM)
        attn_proj = jnp.dot(attn_rows, w_o_flat, preferred_element_type=jnp.float32).astype(jnp.bfloat16)
        resid_rows = (x_blk.astype(jnp.float32) + attn_proj.astype(jnp.float32)).astype(jnp.bfloat16)
        normed_mlp = rms_norm(resid_rows, g_mlp)
        gate_proj = jnp.dot(normed_mlp, w_gate, preferred_element_type=jnp.float32)
        up_proj = jnp.dot(normed_mlp, w_up, preferred_element_type=jnp.float32)
        hidden = (jax.nn.silu(gate_proj) * up_proj).astype(jnp.bfloat16)
        down_proj = jnp.dot(hidden, w_down, preferred_element_type=jnp.float32).astype(jnp.bfloat16)
        return (resid_rows.astype(jnp.float32) + down_proj.astype(jnp.float32)).astype(jnp.bfloat16)

    blocks = lax.map(one_block, (q_all.reshape(n_blocks, Q_BLOCK, N_HEADS, HEAD_DIM),
                                 positions.reshape(n_blocks, Q_BLOCK),
                                 x_rows.reshape(n_blocks, Q_BLOCK, MODEL_DIM)))
    return blocks.reshape(1, SEQ_LEN, MODEL_DIM)
```

```python
import functools
import jax
import jax.numpy as jnp
from jax import lax
from jax.experimental import pallas as pl
from jax.experimental.pallas import tpu as pltpu
from jax.sharding import PartitionSpec as P

NORM_EPS = 1e-5
ROPE_THETA = 500000.0
N_CHUNKS = 4
KEY_BLOCK = 1024
LOG2_E = 1.4426950408889634
REL = (0, 2, 1, 3)


def rms_norm(rows_f32, gain_vec):
    mean_sq = jnp.mean(rows_f32 * rows_f32, axis=-1, keepdims=True)
    return (rows_f32 * lax.rsqrt(mean_sq + NORM_EPS) * gain_vec.astype(jnp.float32)).astype(jnp.bfloat16)


def proj_kernel(a_ref, w0_ref, w1_ref, cos_ref, sin_ref, o_ref, *, rope_heads):
    w = jnp.concatenate([w0_ref[...], w1_ref[...]], axis=1)
    acc = jnp.dot(a_ref[...], w, preferred_element_type=jnp.float32).astype(jnp.bfloat16)
    for h in range(2):
        head = acc[:, h * 128:(h + 1) * 128]
        if h < rope_heads:
            head = head.astype(jnp.float32)
            head = (head * cos_ref[...] + pltpu.roll(head, 64, 1) * sin_ref[...]).astype(jnp.bfloat16)
        o_ref[:, h * 128:(h + 1) * 128] = head


def project(a, w0, w1, first, second, cos, sin, rope_heads, steps):
    rows, depth = a.shape
    cols = steps * 256
    return pl.pallas_call(
        functools.partial(proj_kernel, rope_heads=rope_heads),
        grid=(steps,),
        in_specs=[pl.BlockSpec((rows, depth), lambda n: (0, 0)),
                  pl.BlockSpec((depth, 128), lambda n: (0, first(n))),
                  pl.BlockSpec((depth, 128), lambda n: (0, second(n))),
                  pl.BlockSpec((rows, 128), lambda n: (0, 0)),
                  pl.BlockSpec((rows, 128), lambda n: (0, 0))],
        out_specs=pl.BlockSpec((rows, 256), lambda n: (0, n)),
        out_shape=jax.ShapeDtypeStruct((rows, cols), jnp.bfloat16),
        compiler_params=pltpu.CompilerParams(vmem_limit_bytes=32 * 2**20),
        cost_estimate=pl.CostEstimate(flops=2 * rows * depth * cols, transcendentals=0,
                                      bytes_accessed=2 * (rows * depth + depth * cols + rows * cols)),
    )(a, w0, w1, cos, sin)


def norm_kernel(x_ref, mine_ref, got_ref, gain_ref, resid_ref, b_ref):
    added = (mine_ref[...] + got_ref[...].astype(jnp.float32)).astype(jnp.bfloat16)
    resid = (x_ref[...].astype(jnp.float32) + added.astype(jnp.float32)).astype(jnp.bfloat16)
    resid_ref[...] = resid
    rows = resid.astype(jnp.float32)
    mean_sq = jnp.mean(rows * rows, axis=1, keepdims=True)
    b_ref[...] = (rows * lax.rsqrt(mean_sq + NORM_EPS) * gain_ref[...].astype(jnp.float32)).astype(jnp.bfloat16)


def add_norm(x_rows, mine, got, gain, chunk):
    rows, width = got.shape
    whole = pl.BlockSpec((rows, width), lambda i: (0, 0))
    shape = jax.ShapeDtypeStruct((rows, width), jnp.bfloat16)
    return pl.pallas_call(
        norm_kernel,
        grid=(1,),
        in_specs=[pl.BlockSpec((rows, width), lambda i: (chunk, 0)), whole, whole,
                  pl.BlockSpec((1, width), lambda i: (0, 0))],
        out_specs=[whole, whole],
        out_shape=[shape, shape],
        compiler_params=pltpu.CompilerParams(vmem_limit_bytes=16 * 2**20),
        cost_estimate=pl.CostEstimate(flops=8 * rows * width, transcendentals=rows, bytes_accessed=12 * rows * width),
    )(x_rows, mine, got, gain.reshape(1, width))


def pair_add_kernel(part_ref, got_ref, mine_ref, send_ref):
    rows = mine_ref.shape[0]
    total = part_ref[...].astype(jnp.float32) + got_ref[...].astype(jnp.float32)
    mine_ref[...] = total[:rows]
    send_ref[...] = total[rows:].astype(jnp.bfloat16)


def pair_add(part, got):
    rows, width = part.shape
    block = width // 2
    whole = pl.BlockSpec((rows, block), lambda i: (0, i))
    half = pl.BlockSpec((rows // 2, block), lambda i: (0, i))
    return pl.pallas_call(
        pair_add_kernel,
        grid=(2,),
        in_specs=[whole, whole],
        out_specs=[half, half],
        out_shape=[jax.ShapeDtypeStruct((rows // 2, width), jnp.float32),
                   jax.ShapeDtypeStruct((rows // 2, width), jnp.bfloat16)],
        compiler_params=pltpu.CompilerParams(vmem_limit_bytes=24 * 2**20),
        cost_estimate=pl.CostEstimate(flops=2 * rows * width, transcendentals=0, bytes_accessed=7 * rows * width),
    )(part, got)


def gate_up_kernel(*refs):
    *bs, gate_ref, up_ref, u_ref, b_scr = refs
    rows = bs[0].shape[0]

    @pl.when(pl.program_id(0) == 0)
    def _():
        for i, b in enumerate(bs):
            b_scr[i * rows:(i + 1) * rows, :] = b[...]

    gate = jnp.dot(b_scr[...], gate_ref[...], preferred_element_type=jnp.float32)
    up = jnp.dot(b_scr[...], up_ref[...], preferred_element_type=jnp.float32)
    u_ref[...] = (gate * jax.nn.sigmoid(gate) * up).astype(jnp.bfloat16)


def gate_up(bs, w_gate, w_up):
    rows, width = bs[0].shape
    tall = len(bs) * rows
    hidden = w_gate.shape[1]
    block = 256
    piece = pl.BlockSpec((rows, width), lambda n: (0, 0))
    cols = pl.BlockSpec((width, block), lambda n: (0, n))
    return pl.pallas_call(
        gate_up_kernel,
        grid=(hidden // block,),
        in_specs=[piece] * len(bs) + [cols] * 2,
        out_specs=pl.BlockSpec((tall, block), lambda n: (0, n)),
        out_shape=jax.ShapeDtypeStruct((tall, hidden), jnp.bfloat16),
        scratch_shapes=[pltpu.VMEM((tall, width), jnp.bfloat16)],
        compiler_params=pltpu.CompilerParams(vmem_limit_bytes=63 * 2**20),
        cost_estimate=pl.CostEstimate(flops=4 * tall * width * hidden, transcendentals=tall * hidden,
                                      bytes_accessed=4 * width * hidden + 2 * tall * (width + hidden)),
    )(*bs, w_gate, w_up)


def down_kernel(u_ref, w_ref, *out_refs):
    half = out_refs[0].shape[0]
    out = jnp.dot(u_ref[...], w_ref[...], preferred_element_type=jnp.float32).astype(jnp.bfloat16)
    for i, ref in enumerate(out_refs):
        ref[...] = out[i * half:(i + 1) * half]


def down(u, w_down, first, count, half):
    hidden = u.shape[1]
    width = w_down.shape[1]
    rows = count * half
    block = 512
    out = pl.BlockSpec((half, block), lambda n: (0, n))
    shape = jax.ShapeDtypeStruct((half, width), jnp.bfloat16)
    return pl.pallas_call(
        down_kernel,
        grid=(width // block,),
        in_specs=[pl.BlockSpec((rows, hidden), lambda n: (first, 0)), pl.BlockSpec((hidden, block), lambda n: (0, n))],
        out_specs=[out] * count,
        out_shape=[shape] * count,
        compiler_params=pltpu.CompilerParams(vmem_limit_bytes=63 * 2**20),
        cost_estimate=pl.CostEstimate(flops=2 * rows * width * hidden, transcendentals=0,
                                      bytes_accessed=2 * (width * hidden + rows * (width + hidden))),
    )(u, w_down)


def flash_kernel(info_ref, q0, q1, q2, q3, *rest, rows, chunk, cp_size, dim):
    n_src = 4 * (2 * cp_size - 1)
    sources = rest[:n_src]
    o_p, o_q, kv_scr, q_scr, m_scr, l_scr, acc_scr, sems = rest[n_src:]
    g = pl.program_id(0)
    me, cp = info_ref[0], info_ref[1]
    n_keys = KEY_BLOCK
    heads = 3
    last = 2 * cp_size - 1 - cp

    def each_copy(h, act):
        for i, src in enumerate(sources):
            u, slot = divmod(i, 2 * cp_size - 1)
            j = cp + slot - (cp_size - 1)
            t = me ^ REL[u]
            piece = jnp.where(t < 2, j, 2 * cp_size - 1 - j)

            @pl.when((j >= 0) & (j < cp_size) & (piece <= last))
            def _():
                start = pl.multiple_of(piece * 1024 + (t & 1) * 512, 512)
                act(pltpu.make_async_copy(src.at[:, pl.ds(h * 2 * dim, 2 * dim)], kv_scr.at[h, pl.ds(start, 512)],
                                          sems.at[h, i]))

    @pl.when(g == 0)
    def _():
        each_copy(0, lambda c: c.start())
        each_copy(1, lambda c: c.start())
        each_copy(0, lambda c: c.wait())

    @pl.when(g == 1)
    def _():
        each_copy(1, lambda c: c.wait())

    scale = (dim ** -0.5) * LOG2_E

    def step(first, starts):
        k = kv_scr[g, pl.ds(first, n_keys), 0:dim]
        v = kv_scr[g, pl.ds(first, n_keys), dim:2 * dim]
        s = lax.dot_general(q_scr[...], k, (((1,), (1,)), ((), ())), preferred_element_type=jnp.float32) * scale
        if starts is not None:
            k_pos = first + lax.broadcasted_iota(jnp.int32, (rows, n_keys), 1)
            parts = []
            for i in range(2):
                visible = starts[i] + lax.broadcasted_iota(jnp.int32, (rows, n_keys), 0) >= k_pos
                parts += [jnp.where(visible, s[n * rows:(n + 1) * rows], -1e30) for n in range(i * heads, (i + 1) * heads)]
            s = jnp.concatenate(parts, axis=0)
        m_old = m_scr[...]
        m_new = jnp.maximum(m_old, jnp.max(s, axis=1, keepdims=True))
        m_scr[...] = m_new
        alpha = jnp.exp2(m_old - m_new)
        p = jnp.exp2(s - jnp.tile(m_new, (1, n_keys // 128)))
        part = p[:, 0:128]
        for n in range(1, n_keys // 128):
            part = part + p[:, n * 128:(n + 1) * 128]
        l_scr[...] = l_scr[...] * alpha + part
        acc_scr[...] = acc_scr[...] * alpha + jnp.dot(p.astype(jnp.bfloat16), v, preferred_element_type=jnp.float32)

    for far, q_pair in enumerate(((q0, q2), (q1, q3))):
        t = me ^ (2 * far)
        piece = jnp.where(t < 2, cp, last)
        starts = [piece * 1024 + ((me ^ i) & 1) * 512 + chunk * rows for i in range(2)]
        for i in range(2):
            for h in range(heads):
                n = i * heads + h
                q_scr[n * rows:(n + 1) * rows, :] = q_pair[i][:, h * dim:(h + 1) * dim]
        m_scr[...] = jnp.full_like(m_scr, -1e30)
        l_scr[...] = jnp.zeros_like(l_scr)
        acc_scr[...] = jnp.zeros_like(acc_scr)
        n_full = piece * (1024 // n_keys)

        @pl.loop(0, n_full)
        def _(b):
            step(pl.multiple_of(b * n_keys, n_keys), None)

        @pl.loop(n_full, n_full + 1024 // n_keys)
        def _(b):
            step(pl.multiple_of(b * n_keys, n_keys), starts)

        out = (acc_scr[...] / jnp.sum(l_scr[...], axis=1, keepdims=True)).astype(jnp.bfloat16)
        for i, o_ref in enumerate((o_p, o_q)):
            for h in range(heads):
                n = i * heads + h
                o_ref[far * rows:(far + 1) * rows, h * dim:(h + 1) * dim] = out[n * rows:(n + 1) * rows]


def flash(info, qs, sources, chunk, cp_size):
    rows = qs[0].shape[0] // N_CHUNKS
    dim = 128
    width = 3 * dim
    seq = cp_size * 2048
    q_spec = pl.BlockSpec((rows, width), lambda g: (chunk, g))
    o_spec = pl.BlockSpec((2 * rows, width), lambda g: (0, g))
    o_shape = jax.ShapeDtypeStruct((2 * rows, 2 * width), jnp.bfloat16)
    pairs = 4 * rows * seq // 2
    stat = pltpu.VMEM((6 * rows, 128), jnp.float32)
    return pl.pallas_call(
        functools.partial(flash_kernel, rows=rows, chunk=chunk, cp_size=cp_size, dim=dim),
        grid=(2,),
        in_specs=[pl.BlockSpec(memory_space=pltpu.SMEM)] + [q_spec] * 4 + [pl.BlockSpec(memory_space=pl.ANY)] * len(sources),
        out_specs=[o_spec, o_spec],
        out_shape=[o_shape, o_shape],
        scratch_shapes=[pltpu.VMEM((2, seq, 2 * dim), jnp.bfloat16),
                        pltpu.VMEM((6 * rows, dim), jnp.bfloat16),
                        stat, stat, stat,
                        pltpu.SemaphoreType.DMA((2, len(sources)))],
        compiler_params=pltpu.CompilerParams(vmem_limit_bytes=60 * 2**20),
        cost_estimate=pl.CostEstimate(flops=8 * pairs * 6 * dim, transcendentals=pairs * 6,
                                      bytes_accessed=seq * 4 * dim * 2),
    )(info, *qs, *sources)


def solution(mesh):
    cp_size = mesh.shape['cp']
    row_spec = P('dp', ('cp', 'tp'), None)
    head_cols = P(None, 'tp', None)
    f32, bf16 = jnp.float32, jnp.bfloat16

    def core_swap(v):
        return lax.ppermute(v, 'tp', [(t, t ^ 1) for t in range(4)])

    def y_swap(v):
        return lax.ppermute(v, 'tp', [(t, t ^ 2) for t in range(4)])

    def z_gather(own):
        right, left = own, own
        slots = {0: own}
        for hop in range(1, cp_size):
            right = lax.ppermute(right, 'cp', [(i, i + 1) for i in range(hop - 1, cp_size - 1)])
            left = lax.ppermute(left, 'cp', [(i, i - 1) for i in range(1, cp_size - hop + 1)])
            slots[-hop], slots[hop] = right, left
        return [slots[d] for d in range(1 - cp_size, cp_size)]

    def local_layer(x, g_attn, w_q, w_k, w_v, w_o, g_mlp, w_gate, w_up, w_down):
        x_rows = x[0]
        n_rows, width = x_rows.shape
        me = lax.axis_index('tp')
        cp = lax.axis_index('cp')
        info = jnp.stack([me, cp]).astype(jnp.int32)
        w_q = w_q.reshape(width, -1)
        w_k = w_k.reshape(width, -1)
        w_v = w_v.reshape(width, -1)
        w_o = w_o.reshape(-1, width)

        inv_freq = ROPE_THETA ** (-2.0 * jnp.arange(64, dtype=f32) / 128)
        tables = []
        for rel in REL:
            t = me ^ rel
            start = jnp.where(t < 2, cp, 2 * cp_size - 1 - cp) * 1024 + (t & 1) * 512
            angles = (start + jnp.arange(n_rows, dtype=jnp.int32)).astype(f32)[:, None] * inv_freq[None, :]
            cos, sin = jnp.cos(angles), jnp.sin(angles)
            tables.append((jnp.concatenate([cos, cos], axis=1), jnp.concatenate([-sin, sin], axis=1)))

        a_self = rms_norm(x_rows.astype(f32), g_attn)
        a_y = y_swap(a_self)
        a_core = core_swap(a_self)

        def kv_of(a, i):
            return project(a, w_k, w_v, lambda n: n, lambda n: n, *tables[i], 1, 2)

        def q_of(a, i):
            return project(a, w_q, w_q, lambda n: 2 * n, lambda n: 2 * n + 1, *tables[i], 2, 3)

        kv_self = z_gather(kv_of(a_self, 0))
        kv_core = z_gather(kv_of(a_core, 2))
        q_self = q_of(a_self, 0)
        q_core = q_of(a_core, 2)
        a_diag = core_swap(a_y)
        kv_y = z_gather(kv_of(a_y, 1))
        kv_diag = z_gather(kv_of(a_diag, 3))
        q_y = q_of(a_y, 1)
        q_diag = q_of(a_diag, 3)

        rows = n_rows // N_CHUNKS
        qs = (q_self, q_y, q_core, q_diag)
        sources = tuple(kv_self + kv_y + kv_core + kv_diag)

        def dot(a, b):
            return jnp.dot(a, b, preferred_element_type=f32)

        def after(values, *first):
            return lax.optimization_barrier((values, first))[0]

        def residual(base, mine, got):
            return (base.astype(f32) + (mine + got.astype(f32)).astype(bf16).astype(f32)).astype(bf16)

        resid, b_self, b_y, b_diag = {}, {}, {}, {}
        mine1, got1, mine2, got2 = {}, {}, {}, {}

        def attention(c, *first):
            o_p, o_q = flash(info, after(qs, *first), sources, c, cp_size)
            part_q = dot(o_q, w_o).astype(bf16)
            got = core_swap(part_q)
            mine1[c], send = pair_add(dot(after(o_p, part_q), w_o), got)
            got1[c] = y_swap(send)
            return send

        def spread(c):
            resid[c], b_self[c] = add_norm(x_rows, mine1[c], got1[c], g_mlp, c)
            b_y[c] = y_swap(b_self[c])
            b_diag[c] = core_swap(b_y[c])

        def gate_of(chunks, *first):
            bs = []
            for c in chunks:
                bs += [b_self[c], b_y[c], core_swap(b_self[c]), b_diag[c]]
            return gate_up(after(tuple(bs), *first), w_gate, w_up)

        def return_rows(c, part_p, part_q):
            got = core_swap(part_q)
            mine2[c], send = pair_add(part_p, got)
            got2[c] = y_swap(send)

        sent = attention(0)
        sent = attention(1, sent)
        spread(0)
        sent = attention(2, sent, b_self[0])
        spread(1)
        sent = attention(3, sent, b_self[1])
        spread(2)
        hidden = gate_of((0, 1), sent, b_self[2])
        spread(3)
        parts = down(hidden, w_down, 0, 4, 2 * rows)
        return_rows(0, *parts[:2])
        return_rows(1, *parts[2:])
        hidden = gate_of((2, 3))
        for i in range(2):
            parts = down(hidden, w_down, i, 2, 2 * rows)
            return_rows(2 + i, *parts)
        outs = [residual(resid[c], mine2[c], got2[c]) for c in range(N_CHUNKS)]
        return jnp.concatenate(outs, axis=0)[None]

    return jax.shard_map(local_layer, mesh=mesh,
                         in_specs=(row_spec, P(), head_cols, head_cols, head_cols, P('tp', None, None),
                                   P(), P(None, 'tp'), P(None, 'tp'), P('tp', None)),
                         out_specs=row_spec, check_vma=False)
```

```python
import functools
import jax
import jax.numpy as jnp
from jax import lax
from jax.experimental import pallas as pl
from jax.experimental.pallas import tpu as pltpu
from jax.sharding import PartitionSpec as P

NORM_EPS = 1e-5
ROPE_THETA = 500000.0
N_CHUNKS = 4
KEY_BLOCK = 1024
LOG2_E = 1.4426950408889634
REL = (0, 2, 1, 3)


def rms_norm(rows_f32, gain_vec):
    mean_sq = jnp.mean(rows_f32 * rows_f32, axis=-1, keepdims=True)
    return (rows_f32 * lax.rsqrt(mean_sq + NORM_EPS) * gain_vec.astype(jnp.float32)).astype(jnp.bfloat16)


def proj_kernel(a_ref, w0_ref, w1_ref, cos_ref, sin_ref, o_ref, *, rope_heads):
    w = jnp.concatenate([w0_ref[...], w1_ref[...]], axis=1)
    acc = jnp.dot(a_ref[...], w, preferred_element_type=jnp.float32).astype(jnp.bfloat16)
    for h in range(2):
        head = acc[:, h * 128:(h + 1) * 128]
        if h < rope_heads:
            head = head.astype(jnp.float32)
            head = (head * cos_ref[...] + pltpu.roll(head, 64, 1) * sin_ref[...]).astype(jnp.bfloat16)
        o_ref[:, h * 128:(h + 1) * 128] = head


def project(a, w0, w1, first, second, cos, sin, rope_heads, steps):
    rows, depth = a.shape
    cols = steps * 256
    return pl.pallas_call(
        functools.partial(proj_kernel, rope_heads=rope_heads),
        grid=(steps,),
        in_specs=[pl.BlockSpec((rows, depth), lambda n: (0, 0)),
                  pl.BlockSpec((depth, 128), lambda n: (0, first(n))),
                  pl.BlockSpec((depth, 128), lambda n: (0, second(n))),
                  pl.BlockSpec((rows, 128), lambda n: (0, 0)),
                  pl.BlockSpec((rows, 128), lambda n: (0, 0))],
        out_specs=pl.BlockSpec((rows, 256), lambda n: (0, n)),
        out_shape=jax.ShapeDtypeStruct((rows, cols), jnp.bfloat16),
        compiler_params=pltpu.CompilerParams(vmem_limit_bytes=32 * 2**20),
        cost_estimate=pl.CostEstimate(flops=2 * rows * depth * cols, transcendentals=0,
                                      bytes_accessed=2 * (rows * depth + depth * cols + rows * cols)),
    )(a, w0, w1, cos, sin)


def norm_kernel(x_ref, mine_ref, got_ref, gain_ref, resid_ref, b_ref):
    added = (mine_ref[...] + got_ref[...].astype(jnp.float32)).astype(jnp.bfloat16)
    resid = (x_ref[...].astype(jnp.float32) + added.astype(jnp.float32)).astype(jnp.bfloat16)
    resid_ref[...] = resid
    rows = resid.astype(jnp.float32)
    mean_sq = jnp.mean(rows * rows, axis=1, keepdims=True)
    b_ref[...] = (rows * lax.rsqrt(mean_sq + NORM_EPS) * gain_ref[...].astype(jnp.float32)).astype(jnp.bfloat16)


def add_norm(x_rows, mine, got, gain, chunk):
    rows, width = got.shape
    whole = pl.BlockSpec((rows, width), lambda i: (0, 0))
    shape = jax.ShapeDtypeStruct((rows, width), jnp.bfloat16)
    return pl.pallas_call(
        norm_kernel,
        grid=(1,),
        in_specs=[pl.BlockSpec((rows, width), lambda i: (chunk, 0)), whole, whole,
                  pl.BlockSpec((1, width), lambda i: (0, 0))],
        out_specs=[whole, whole],
        out_shape=[shape, shape],
        compiler_params=pltpu.CompilerParams(vmem_limit_bytes=16 * 2**20),
        cost_estimate=pl.CostEstimate(flops=8 * rows * width, transcendentals=rows, bytes_accessed=12 * rows * width),
    )(x_rows, mine, got, gain.reshape(1, width))


def pair_add_kernel(part_ref, got_ref, mine_ref, send_ref):
    rows = mine_ref.shape[0]
    total = part_ref[...].astype(jnp.float32) + got_ref[...].astype(jnp.float32)
    mine_ref[...] = total[:rows]
    send_ref[...] = total[rows:].astype(jnp.bfloat16)


def pair_add(part, got):
    rows, width = part.shape
    block = width // 2
    whole = pl.BlockSpec((rows, block), lambda i: (0, i))
    half = pl.BlockSpec((rows // 2, block), lambda i: (0, i))
    return pl.pallas_call(
        pair_add_kernel,
        grid=(2,),
        in_specs=[whole, whole],
        out_specs=[half, half],
        out_shape=[jax.ShapeDtypeStruct((rows // 2, width), jnp.float32),
                   jax.ShapeDtypeStruct((rows // 2, width), jnp.bfloat16)],
        compiler_params=pltpu.CompilerParams(vmem_limit_bytes=24 * 2**20),
        cost_estimate=pl.CostEstimate(flops=2 * rows * width, transcendentals=0, bytes_accessed=7 * rows * width),
    )(part, got)


def gate_up_kernel(*refs):
    *bs, gate_ref, up_ref, u_ref, b_scr = refs
    rows = bs[0].shape[0]

    @pl.when(pl.program_id(0) == 0)
    def _():
        for i, b in enumerate(bs):
            b_scr[i * rows:(i + 1) * rows, :] = b[...]

    gate = jnp.dot(b_scr[...], gate_ref[...], preferred_element_type=jnp.float32)
    up = jnp.dot(b_scr[...], up_ref[...], preferred_element_type=jnp.float32)
    u_ref[...] = (gate * jax.nn.sigmoid(gate) * up).astype(jnp.bfloat16)


def gate_up(bs, w_gate, w_up):
    rows, width = bs[0].shape
    tall = len(bs) * rows
    hidden = w_gate.shape[1]
    block = 256
    piece = pl.BlockSpec((rows, width), lambda n: (0, 0))
    cols = pl.BlockSpec((width, block), lambda n: (0, n))
    return pl.pallas_call(
        gate_up_kernel,
        grid=(hidden // block,),
        in_specs=[piece] * len(bs) + [cols] * 2,
        out_specs=pl.BlockSpec((tall, block), lambda n: (0, n)),
        out_shape=jax.ShapeDtypeStruct((tall, hidden), jnp.bfloat16),
        scratch_shapes=[pltpu.VMEM((tall, width), jnp.bfloat16)],
        compiler_params=pltpu.CompilerParams(vmem_limit_bytes=63 * 2**20),
        cost_estimate=pl.CostEstimate(flops=4 * tall * width * hidden, transcendentals=tall * hidden,
                                      bytes_accessed=4 * width * hidden + 2 * tall * (width + hidden)),
    )(*bs, w_gate, w_up)


def down_kernel(u_ref, w_ref, *out_refs):
    half = out_refs[0].shape[0]
    out = jnp.dot(u_ref[...], w_ref[...], preferred_element_type=jnp.float32).astype(jnp.bfloat16)
    for i, ref in enumerate(out_refs):
        ref[...] = out[i * half:(i + 1) * half]


def down(u, w_down, first, count, half):
    hidden = u.shape[1]
    width = w_down.shape[1]
    rows = count * half
    block = 512
    out = pl.BlockSpec((half, block), lambda n: (0, n))
    shape = jax.ShapeDtypeStruct((half, width), jnp.bfloat16)
    return pl.pallas_call(
        down_kernel,
        grid=(width // block,),
        in_specs=[pl.BlockSpec((rows, hidden), lambda n: (first, 0)), pl.BlockSpec((hidden, block), lambda n: (0, n))],
        out_specs=[out] * count,
        out_shape=[shape] * count,
        compiler_params=pltpu.CompilerParams(vmem_limit_bytes=63 * 2**20),
        cost_estimate=pl.CostEstimate(flops=2 * rows * width * hidden, transcendentals=0,
                                      bytes_accessed=2 * (width * hidden + rows * (width + hidden))),
    )(u, w_down)


def flash_kernel(info_ref, q0, q1, q2, q3, w_ref, *rest, rows, chunk, cp_size, dim):
    n_src = 4 * (2 * cp_size - 1)
    sources = rest[:n_src]
    part_p, part_q, kv_scr, q_scr, m_scr, l_scr, acc_scr, o_scr, w_scr, sems, w_sem = rest[n_src:]
    w_copy = pltpu.make_async_copy(w_ref, w_scr, w_sem)
    g = pl.program_id(0)
    me, cp = info_ref[0], info_ref[1]
    n_keys = KEY_BLOCK
    heads = 3
    last = 2 * cp_size - 1 - cp

    def each_copy(h, act):
        for i, src in enumerate(sources):
            u, slot = divmod(i, 2 * cp_size - 1)
            j = cp + slot - (cp_size - 1)
            t = me ^ REL[u]
            piece = jnp.where(t < 2, j, 2 * cp_size - 1 - j)

            @pl.when((j >= 0) & (j < cp_size) & (piece <= last))
            def _():
                start = pl.multiple_of(piece * 1024 + (t & 1) * 512, 512)
                act(pltpu.make_async_copy(src.at[:, pl.ds(h * 2 * dim, 2 * dim)], kv_scr.at[h, pl.ds(start, 512)],
                                          sems.at[h, i]))

    @pl.when(g == 0)
    def _():
        each_copy(0, lambda c: c.start())
        each_copy(1, lambda c: c.start())
        w_copy.start()
        each_copy(0, lambda c: c.wait())

    @pl.when(g == 1)
    def _():
        each_copy(1, lambda c: c.wait())

    scale = (dim ** -0.5) * LOG2_E

    def step(first, starts):
        k = kv_scr[g, pl.ds(first, n_keys), 0:dim]
        v = kv_scr[g, pl.ds(first, n_keys), dim:2 * dim]
        s = lax.dot_general(q_scr[...], k, (((1,), (1,)), ((), ())), preferred_element_type=jnp.float32) * scale
        if starts is not None:
            k_pos = first + lax.broadcasted_iota(jnp.int32, (rows, n_keys), 1)
            parts = []
            for i in range(2):
                visible = starts[i] + lax.broadcasted_iota(jnp.int32, (rows, n_keys), 0) >= k_pos
                parts += [jnp.where(visible, s[n * rows:(n + 1) * rows], -1e30) for n in range(i * heads, (i + 1) * heads)]
            s = jnp.concatenate(parts, axis=0)
        m_old = m_scr[...]
        m_new = jnp.maximum(m_old, jnp.max(s, axis=1, keepdims=True))
        m_scr[...] = m_new
        alpha = jnp.exp2(m_old - m_new)
        p = jnp.exp2(s - jnp.tile(m_new, (1, n_keys // 128)))
        part = p[:, 0:128]
        for n in range(1, n_keys // 128):
            part = part + p[:, n * 128:(n + 1) * 128]
        l_scr[...] = l_scr[...] * alpha + part
        acc_scr[...] = acc_scr[...] * alpha + jnp.dot(p.astype(jnp.bfloat16), v, preferred_element_type=jnp.float32)

    @pl.loop(0, 2)
    def _(far):
        for side, q_pair in enumerate(((q0, q2), (q1, q3))):
            @pl.when(far == side)
            def _():
                for i in range(2):
                    for h in range(heads):
                        n = i * heads + h
                        q_scr[n * rows:(n + 1) * rows, :] = q_pair[i][:, h * dim:(h + 1) * dim]

        t = me ^ (2 * far)
        piece = jnp.where(t < 2, cp, last)
        starts = [piece * 1024 + ((me ^ i) & 1) * 512 + chunk * rows for i in range(2)]
        m_scr[...] = jnp.full_like(m_scr, -1e30)
        l_scr[...] = jnp.zeros_like(l_scr)
        acc_scr[...] = jnp.zeros_like(acc_scr)
        n_full = piece * (1024 // n_keys)

        @pl.loop(0, n_full)
        def _(b):
            step(pl.multiple_of(b * n_keys, n_keys), None)

        @pl.loop(n_full, n_full + 1024 // n_keys)
        def _(b):
            step(pl.multiple_of(b * n_keys, n_keys), starts)

        out = (acc_scr[...] / jnp.sum(l_scr[...], axis=1, keepdims=True)).astype(jnp.bfloat16)
        for i in range(2):
            row = pl.multiple_of(i * 2 * rows + far * rows, rows)
            for h in range(heads):
                n = i * heads + h
                o_scr[g, pl.ds(row, rows), h * dim:(h + 1) * dim] = out[n * rows:(n + 1) * rows]

    @pl.when(g == 1)
    def _():
        w_copy.wait()

        @pl.loop(0, w_scr.shape[1] // 512)
        def _(n):
            cols = pl.ds(pl.multiple_of(n * 512, 512), 512)
            part = jnp.dot(o_scr[0], w_scr[:heads * dim, cols], preferred_element_type=jnp.float32)
            part = part + jnp.dot(o_scr[1], w_scr[heads * dim:, cols], preferred_element_type=jnp.float32)
            part_p[:, cols] = part[:2 * rows].astype(jnp.bfloat16)
            part_q[:, cols] = part[2 * rows:].astype(jnp.bfloat16)


def flash(info, qs, w_o, sources, chunk, cp_size):
    rows = qs[0].shape[0] // N_CHUNKS
    dim = 128
    width = 3 * dim
    seq = cp_size * 2048
    q_spec = pl.BlockSpec((rows, width), lambda g: (chunk, g))
    model = w_o.shape[1]
    o_spec = pl.BlockSpec((2 * rows, model), lambda g: (0, 0))
    o_shape = jax.ShapeDtypeStruct((2 * rows, model), jnp.bfloat16)
    pairs = 4 * rows * seq // 2
    stat = pltpu.VMEM((6 * rows, 128), jnp.float32)
    return pl.pallas_call(
        functools.partial(flash_kernel, rows=rows, chunk=chunk, cp_size=cp_size, dim=dim),
        grid=(2,),
        in_specs=[pl.BlockSpec(memory_space=pltpu.SMEM)] + [q_spec] * 4 + [pl.BlockSpec(memory_space=pl.ANY)] * (1 + len(sources)),
        out_specs=[o_spec, o_spec],
        out_shape=[o_shape, o_shape],
        scratch_shapes=[pltpu.VMEM((2, seq, 2 * dim), jnp.bfloat16),
                        pltpu.VMEM((6 * rows, dim), jnp.bfloat16),
                        stat, stat, stat,
                        pltpu.VMEM((2, 4 * rows, width), jnp.bfloat16),
                        pltpu.VMEM(w_o.shape, jnp.bfloat16),
                        pltpu.SemaphoreType.DMA((2, len(sources))),
                        pltpu.SemaphoreType.DMA],
        compiler_params=pltpu.CompilerParams(vmem_limit_bytes=60 * 2**20),
        cost_estimate=pl.CostEstimate(flops=8 * pairs * 6 * dim, transcendentals=pairs * 6,
                                      bytes_accessed=seq * 4 * dim * 2),
    )(info, *qs, w_o, *sources)


def solution(mesh):
    cp_size = mesh.shape['cp']
    row_spec = P('dp', ('cp', 'tp'), None)
    head_cols = P(None, 'tp', None)
    f32, bf16 = jnp.float32, jnp.bfloat16

    def core_swap(v):
        return lax.ppermute(v, 'tp', [(t, t ^ 1) for t in range(4)])

    def y_swap(v):
        return lax.ppermute(v, 'tp', [(t, t ^ 2) for t in range(4)])

    def z_gather(own):
        right, left = own, own
        slots = {0: own}
        for hop in range(1, cp_size):
            right = lax.ppermute(right, 'cp', [(i, i + 1) for i in range(hop - 1, cp_size - 1)])
            left = lax.ppermute(left, 'cp', [(i, i - 1) for i in range(1, cp_size - hop + 1)])
            slots[-hop], slots[hop] = right, left
        return [slots[d] for d in range(1 - cp_size, cp_size)]

    def local_layer(x, g_attn, w_q, w_k, w_v, w_o, g_mlp, w_gate, w_up, w_down):
        x_rows = x[0]
        n_rows, width = x_rows.shape
        me = lax.axis_index('tp')
        cp = lax.axis_index('cp')
        info = jnp.stack([me, cp]).astype(jnp.int32)
        w_q = w_q.reshape(width, -1)
        w_k = w_k.reshape(width, -1)
        w_v = w_v.reshape(width, -1)
        w_o = w_o.reshape(-1, width)

        inv_freq = ROPE_THETA ** (-2.0 * jnp.arange(64, dtype=f32) / 128)
        tables = []
        for rel in REL:
            t = me ^ rel
            start = jnp.where(t < 2, cp, 2 * cp_size - 1 - cp) * 1024 + (t & 1) * 512
            angles = (start + jnp.arange(n_rows, dtype=jnp.int32)).astype(f32)[:, None] * inv_freq[None, :]
            cos, sin = jnp.cos(angles), jnp.sin(angles)
            tables.append((jnp.concatenate([cos, cos], axis=1), jnp.concatenate([-sin, sin], axis=1)))

        a_self = rms_norm(x_rows.astype(f32), g_attn)
        a_y = y_swap(a_self)
        a_core = core_swap(a_self)

        def kv_of(a, i):
            return project(a, w_k, w_v, lambda n: n, lambda n: n, *tables[i], 1, 2)

        def q_of(a, i):
            return project(a, w_q, w_q, lambda n: 2 * n, lambda n: 2 * n + 1, *tables[i], 2, 3)

        kv_self = z_gather(kv_of(a_self, 0))
        kv_core = z_gather(kv_of(a_core, 2))
        q_self = q_of(a_self, 0)
        q_core = q_of(a_core, 2)
        a_diag = core_swap(a_y)
        kv_y = z_gather(kv_of(a_y, 1))
        kv_diag = z_gather(kv_of(a_diag, 3))
        q_y = q_of(a_y, 1)
        q_diag = q_of(a_diag, 3)

        rows = n_rows // N_CHUNKS
        qs = (q_self, q_y, q_core, q_diag)
        sources = tuple(kv_self + kv_y + kv_core + kv_diag)

        def after(values, *first):
            return lax.optimization_barrier((values, first))[0]

        def residual(base, mine, got):
            return (base.astype(f32) + (mine + got.astype(f32)).astype(bf16).astype(f32)).astype(bf16)

        resid, b_self, b_y, b_diag = {}, {}, {}, {}
        mine1, got1, mine2, got2 = {}, {}, {}, {}

        def attention(c, *first):
            part_p, part_q = flash(info, after(qs, *first), w_o, sources, c, cp_size)
            got = core_swap(part_q)
            mine1[c], send = pair_add(part_p, got)
            got1[c] = y_swap(send)
            return send

        def spread(c):
            resid[c], b_self[c] = add_norm(x_rows, mine1[c], got1[c], g_mlp, c)
            b_y[c] = y_swap(b_self[c])
            b_diag[c] = core_swap(b_y[c])

        def gate_of(chunks, *first):
            bs = []
            for c in chunks:
                bs += [b_self[c], b_y[c], core_swap(b_self[c]), b_diag[c]]
            return gate_up(after(tuple(bs), *first), w_gate, w_up)

        def return_rows(c, part_p, part_q):
            got = core_swap(part_q)
            mine2[c], send = pair_add(part_p, got)
            got2[c] = y_swap(send)

        sent = attention(0)
        sent = attention(1, sent)
        spread(0)
        sent = attention(2, sent, b_self[0])
        spread(1)
        sent = attention(3, sent, b_self[1])
        spread(2)
        hidden = gate_of((0, 1), sent, b_self[2])
        spread(3)
        parts = down(hidden, w_down, 0, 4, 2 * rows)
        return_rows(0, *parts[:2])
        return_rows(1, *parts[2:])
        hidden = gate_of((2, 3))
        for i in range(2):
            parts = down(hidden, w_down, i, 2, 2 * rows)
            return_rows(2 + i, *parts)
        outs = [residual(resid[c], mine2[c], got2[c]) for c in range(N_CHUNKS)]
        return jnp.concatenate(outs, axis=0)[None]

    return jax.shard_map(local_layer, mesh=mesh,
                         in_specs=(row_spec, P(), head_cols, head_cols, head_cols, P('tp', None, None),
                                   P(), P(None, 'tp'), P(None, 'tp'), P('tp', None)),
                         out_specs=row_spec, check_vma=False)
```
